8 devices in a mesh: dp: 2 (over z, y), tp: 4 (over x, core).
Axes of the slice: x: 2, y: 2, z: 1, core: 2. Of those that a mesh axis runs over, the one named last changes fastest.
Arguments:
- w_up: bfloat16 [2, 2560, 10240], P(None, None, 'tp')
- w_down: bfloat16 [2, 10240, 2560], P(None, 'tp')
- saved_x: bfloat16 [2, 2, 4096, 2560], P(None, 'dp')
- saved_h: bfloat16 [2, 2, 4096, 10240], P(None, 'dp', None, 'tp')
- grad_out: bfloat16 [2, 4096, 2560], P('dp')
Outputs:
- output 1: bfloat16 [2, 4096, 2560], P('dp')
- output 2: float32 [2, 2560, 10240], P(None, 'dp', 'tp')
- output 3: float32 [2, 10240, 2560], P(None, 'tp', 'dp')
All inputs are finite; a program needn't handle non-finite values.
Results may differ from the reference program's by a relative error of at most 0.014246.
Values are sent between devices in bfloat16 or wider.
A program may use at most 1 GiB of HBM per device.

```python
import jax
import jax.numpy as jnp
import math
from jax import lax

D = 2560
FF = 10240
BATCH_DEV = 1
DATA = 2
SEQ = 4096
LAYERS = 2

BATCH = BATCH_DEV * DATA
GELU_SCALE = math.sqrt(2.0 / math.pi)
GELU_CUBIC = 0.044715


def gelu_and_slope(pre_act):
    tanh_val = jnp.tanh(GELU_SCALE * (pre_act + GELU_CUBIC * pre_act * pre_act * pre_act))
    act_val = 0.5 * pre_act * (1.0 + tanh_val)
    act_slope = 0.5 * (1.0 + tanh_val) + 0.5 * pre_act * (1.0 - tanh_val * tanh_val) * GELU_SCALE * (1.0 + 3.0 * GELU_CUBIC * pre_act * pre_act)
    return act_val, act_slope


def forward_saved(w_up, w_down, x_first):
    x_list = []
    h_list = []
    x_cur = x_first
    for layer_idx in range(LAYERS):
        h_cur = jnp.dot(x_cur, w_up[layer_idx], preferred_element_type=jnp.float32).astype(jnp.bfloat16)
        act_val = gelu_and_slope(h_cur.astype(jnp.float32))[0]
        branch = jnp.dot(act_val.astype(jnp.bfloat16), w_down[layer_idx], preferred_element_type=jnp.float32)
        x_list.append(x_cur)
        h_list.append(h_cur)
        x_cur = (x_cur.astype(jnp.float32) + branch).astype(jnp.bfloat16)
    saved_x = jnp.stack(x_list).reshape(LAYERS, BATCH, SEQ, D)
    saved_h = jnp.stack(h_list).reshape(LAYERS, BATCH, SEQ, FF)
    return saved_x, saved_h


def setup_inputs(seed: int = 0) -> dict:
    key_list = jax.random.split(jax.random.key(seed), 4)
    token_count = BATCH * SEQ
    w_up = (jax.random.normal(key_list[0], (LAYERS, D, FF), jnp.float32) * (D ** -0.5)).astype(jnp.bfloat16)
    w_down = (jax.random.normal(key_list[1], (LAYERS, FF, D), jnp.float32) * (1.5 * FF ** -0.5)).astype(jnp.bfloat16)
    x_first = jax.random.normal(key_list[2], (token_count, D), jnp.float32).astype(jnp.bfloat16)
    grad_out = (jax.random.normal(key_list[3], (BATCH, SEQ, D), jnp.float32) * (token_count ** -0.5)).astype(jnp.bfloat16)
    saved_x, saved_h = forward_saved(w_up, w_down, x_first)
    return {"w_up": w_up, "w_down": w_down, "saved_x": saved_x, "saved_h": saved_h, "grad_out": grad_out}


def block_backward(w_up, w_down, x_rows, h_rows, grad_rows):
    grad_cur = grad_rows
    up_list = []
    down_list = []
    for layer_idx in reversed(range(LAYERS)):
        act_val, act_slope = gelu_and_slope(h_rows[layer_idx].astype(jnp.float32))
        d_act = jnp.dot(grad_cur, w_down[layer_idx].T, preferred_element_type=jnp.float32)
        d_pre = (d_act * act_slope).astype(jnp.bfloat16)
        back_sum = jnp.dot(d_pre, w_up[layer_idx].T, preferred_element_type=jnp.float32)
        down_list.append(jnp.dot(act_val.astype(jnp.bfloat16).T, grad_cur, preferred_element_type=jnp.float32))
        up_list.append(jnp.dot(x_rows[layer_idx].T, d_pre, preferred_element_type=jnp.float32))
        grad_cur = (grad_cur.astype(jnp.float32) + back_sum).astype(jnp.bfloat16)
    return grad_cur, jnp.stack(up_list[::-1]), jnp.stack(down_list[::-1])


def reference(w_up, w_down, saved_x, saved_h, grad_out):
    row_count = BATCH_DEV * SEQ
    x_blocks = jnp.swapaxes(saved_x.reshape(LAYERS, DATA, row_count, D), 0, 1)
    h_blocks = jnp.swapaxes(saved_h.reshape(LAYERS, DATA, row_count, FF), 0, 1)
    g_blocks = grad_out.reshape(DATA, row_count, D)

    def body(carry_in, block_in):
        up_sum, down_sum = carry_in
        grad_in, up_part, down_part = block_backward(w_up, w_down, block_in[0], block_in[1], block_in[2])
        return (up_sum + up_part, down_sum + down_part), grad_in

    init_carry = (jnp.zeros((LAYERS, D, FF), jnp.float32), jnp.zeros((LAYERS, FF, D), jnp.float32))
    sums_out, grad_blocks = lax.scan(body, init_carry, (x_blocks, h_blocks, g_blocks))
    return grad_blocks.reshape(BATCH, SEQ, D), sums_out[0], sums_out[1]
```

```python
import math

import jax
import jax.numpy as jnp
from jax import lax
from jax.experimental import pallas as pl
from jax.experimental.pallas import tpu as pltpu
from jax.sharding import PartitionSpec as P

C0 = math.sqrt(2.0 / math.pi)
C1 = 0.044715
F32, BF16 = jnp.float32, jnp.bfloat16
ANY = pl.BlockSpec(memory_space=pl.ANY)
VMEM_LIMIT = 67043328
BM = 512


def gelu_and_slope(h):
    sq = h * h
    q = 0.5 + 0.5 * jnp.tanh(h * (C0 + (C0 * C1) * sq))
    act = h * q
    return act, q + act * (1.0 - q) * (2.0 * C0 + (6.0 * C0 * C1) * sq)


def dot(a, b, ca, cb):
    return lax.dot_general(a, b, (((ca,), (cb,)), ((), ())), preferred_element_type=F32)


def dw_step(kind, acc, lr, rr):
    n = acc.shape[1]
    for i in range(2):
        at = slice(i * n, i * n + n)
        if kind == "up":
            acc[i] += dot(lr[...], rr[:, at], 0, 0)
        else:
            acc[i] += dot(lr[:, at], rr[...], 0, 0)


def halves(kind, ref, i, n):
    at = pl.ds(i * n, n)
    return ref.at[:, at] if kind == "up" else ref.at[at]


def main_kernel(
    w_up, w_down, xs, hs, g2,
    g0, g1, dh, aa, ps, r1, r2, xp1, gp2, xp0, gp1, dhp, ap, down1, up1, down0, up0,
    wu, wd, acc, wsem, asem, send, recv,
):
    tokens, width = g2.shape[1:]
    dp, tp = lax.axis_index("dp"), lax.axis_index("tp")
    c, x = lax.rem(tp, 2), lax.div(tp, 2)
    Y, X, C = (1 - dp, tp), (dp, (1 - x) * 2 + c), (dp, x * 2 + (1 - c))
    half = tokens // 2
    quarter = tokens // 4
    sub = quarter // 2
    NB = width // 2

    barrier = pltpu.get_barrier_semaphore()
    for peer in (Y, X, C):
        pl.semaphore_signal(barrier, inc=1, device_id=peer, device_id_type=pl.DeviceIdType.MESH)
    pl.semaphore_wait(barrier, 3)

    slot = {}

    def rc(name, src, dst, to, s=0, n=1):
        if name not in slot:
            slot[name] = sum(v[1] for v in slot.values()), n
        i = slot[name][0] + s
        return pltpu.make_async_remote_copy(
            src_ref=src, dst_ref=dst, send_sem=send.at[i], recv_sem=recv.at[i],
            device_id=to, device_id_type=pl.DeviceIdType.MESH)

    def at_rows(ref, start, size):
        return ref.at[pl.ds(pl.multiple_of(start, sub), size)]

    def qrow(cc, xx, s):
        return cc * half + xx * quarter + s * sub

    def same(name, src, dst, row, to, s=0, n=1):
        return rc(name, at_rows(src, row, sub), at_rows(dst, row, sub), to, s, n)

    def k_row(k):
        return c * half + k * sub

    x1, x0, gtop = xs.at[1, 0], xs.at[0, 0], g2.at[0]

    def kx(k):
        return same(f"kx{k}", x1, xp1, k_row(k), Y)

    def kg(k):
        return same(f"kg{k}", gtop, gp2, k_row(k), Y)

    def fkx(k):
        return same(f"fkx{k}", xp1, xp1, k_row(k), C)

    def fkg(k):
        return same(f"fkg{k}", gp2, gp2, k_row(k), C)

    def share(tag, src, dst):
        return {
            "y": lambda s: same(f"{tag}y{s}", src, dst, qrow(c, x, s), Y),
            "x": lambda s: same(f"{tag}x{s}", dst, dst, qrow(c, x, s), X),
            "c": lambda s: same(f"{tag}c{s}", dst, dst, qrow(c, x, s), C),
            "f": lambda s: same(f"{tag}f{s}", dst, dst, qrow(c, 1 - x, s), C),
        }

    sx0 = share("sx0", x0, xp0)
    sg1 = share("sg1", g1, gp1)

    def gather(tag, g):
        return {
            "x": lambda s: same(f"{tag}x{s}", g, g, qrow(c, x, s), X),
            "c": lambda s: same(f"{tag}c{s}", g, g, qrow(c, x, s), C),
            "f": lambda s: same(f"{tag}f{s}", g, g, qrow(c, 1 - x, s), C),
        }

    ag = {1: gather("ag1", g1), 0: gather("ag0", g0)}

    def r1_copy(l, pair):
        xx = jnp.where(pair < 2, 1 - x, x)
        s = lax.rem(pair, 2)
        return rc(f"r1_{l}", at_rows(ps.at[l], qrow(1 - c, xx, s), sub),
                  at_rows(r1.at[l], xx * quarter + s * sub, sub), C, pair, 4)

    def r2_copy(l, s):
        return rc(f"r2_{l}", at_rows(ps.at[l], qrow(c, 1 - x, s), sub),
                  at_rows(r2.at[l], s * sub, sub), X, s, 2)

    def load(l, which):
        src, dst, i = (w_up, wu, 0) if which == "up" else (w_down, wd, 1)
        return pltpu.make_async_copy(src.at[l], dst, wsem.at[i])

    def d_act(l, g, blk):
        def body(gr, hr, dr, ar):
            n = pl.program_id(1)
            d = dot(gr[...], wd[pl.ds(pl.multiple_of(n * NB, NB), NB), :], 1, 1)
            act, slope = gelu_and_slope(hr[...].astype(F32))
            dr[...] = (d * slope).astype(BF16)
            ar[...] = act.astype(BF16)

        tile = pl.BlockSpec((BM, NB), lambda i, n: (blk + i, n))
        pltpu.emit_pipeline(
            body, grid=(1, 2),
            in_specs=[pl.BlockSpec((BM, width), lambda i, n: (blk + i, 0)), tile],
            out_specs=[tile, tile],
        )(g, hs.at[l, 0], dh.at[l], aa.at[l])

    def d_x(l, blk, add_blk=None):
        def body(dr, *rest):
            n = pl.program_id(1)
            out = dot(dr[...], wu[pl.ds(pl.multiple_of(n * NB, NB), NB), :], 1, 1)
            if len(rest) == 2:
                out = out + rest[0][...].astype(F32)
            rest[-1][...] = out.astype(BF16)

        tile = pl.BlockSpec((BM, NB), lambda i, n: (blk + i, n))
        ins = [pl.BlockSpec((BM, width), lambda i, n: (blk + i, 0))]
        refs = [dh.at[l]]
        if add_blk is not None:
            ins.append(pl.BlockSpec((BM, NB), lambda i, n: (add_blk + i, n)))
            refs.append(r1.at[l])
        pltpu.emit_pipeline(body, grid=(1, 2), in_specs=ins, out_specs=[tile])(*refs, ps.at[l])

    def own(l, g, hook):
        def pair_step(pair, _):
            xx = jnp.where(pair < 2, 1 - x, x)
            s = lax.rem(pair, 2)
            other = (1 - c) * 4 + xx * 2 + s
            mine = c * 4 + xx * 2 + s

            def step(j, _):
                blk = jnp.where(j == 0, other, mine)
                if l == 0:
                    @pl.when(jnp.logical_and(pair < 2, j == 0))
                    def _():
                        @pl.when(s == 0)
                        def _():
                            ag[1]["f"](0).wait_recv()

                        @pl.when(s == 1)
                        def _():
                            ag[1]["f"](1).wait_recv()
                d_act(l, g, blk)

                @pl.when(j == 0)
                def _():
                    d_x(l, blk)
                    r1_copy(l, pair).start()

                @pl.when(j == 1)
                def _():
                    r1_copy(l, pair).wait_recv()
                    d_x(l, blk, xx * 2 + s)

                    @pl.when(pair < (2 if l == 1 else 1))
                    def _():
                        r2_copy(l, s).start()
                return 0

            lax.fori_loop(0, 2, step, 0)
            for p in range(4):
                @pl.when(pair == p)
                def _():
                    hook(p)
            return 0

        lax.fori_loop(0, 4, pair_step, 0)

    QB = 128

    def add_quarter(l, g, out, s):
        r2_copy(l, s).wait_recv()
        base = lax.div(qrow(c, x, s), QB)

        def body(gr, pr, rr, orf):
            orf[...] = (gr[...].astype(F32) + (pr[...].astype(F32) + rr[...].astype(F32))).astype(BF16)

        at = pl.BlockSpec((QB, width), lambda i: (base + i, 0))
        pltpu.emit_pipeline(
            body, grid=(sub // QB,),
            in_specs=[at, at, pl.BlockSpec((QB, width), lambda i: (s * (sub // QB) + i, 0))],
            out_specs=[at],
        )(g, ps.at[l], r2.at[l], out)
        ag[l]["c"](s).start()

    def peer(l, px, pg, blocks, row_block):
        def body(xr, gr, dr, ar):
            n = pl.program_id(1)
            t = pl.ds(pl.multiple_of(n * NB, NB), NB)
            pre = dot(xr[...], wu[:, t], 1, 0).astype(BF16)
            act, slope = gelu_and_slope(pre.astype(F32))
            ar[...] = act.astype(BF16)
            dr[...] = (dot(gr[...], wd[t, :], 1, 1) * slope).astype(BF16)

        full = pl.BlockSpec((BM, width), lambda i, n: (row_block(i), 0))
        tile = pl.BlockSpec((BM, NB), lambda i, n: (row_block(i), n))
        pltpu.emit_pipeline(body, grid=(blocks, 2), in_specs=[full, full], out_specs=[tile, tile])(
            px, pg, dhp.at[l], ap.at[l])

    def acc_copies(kind, ref, out):
        res = []
        for i in range(2):
            far = halves(kind, ref, i, NB) if kind else ref.at[i]
            pair = (acc.at[i], far) if out else (far, acc.at[i])
            res.append(pltpu.make_async_copy(*pair, asem.at[i]))
        return res

    def weights(kind, dst, init, lhs, rhs, blocks, row_block, final=True):
        lay = kind if final else None
        if init:
            for cp in acc_copies(lay, dst, False):
                cp.start()
            for cp in acc_copies(lay, dst, False):
                cp.wait()
        else:
            acc[...] = jnp.zeros_like(acc)
        lw, rw = (NB, width) if kind == "up" else (width, NB)
        lcol, rcol = (dp, 0) if kind == "up" else (0, dp)
        pltpu.emit_pipeline(
            lambda lr, rr: dw_step(kind, acc, lr, rr),
            grid=(blocks,),
            in_specs=[
                pl.BlockSpec((BM, lw), lambda i: (row_block(i), lcol)),
                pl.BlockSpec((BM, rw), lambda i: (row_block(i), rcol)),
            ],
        )(lhs, rhs)
        for cp in acc_copies(lay, dst, True):
            cp.start()
        for cp in acc_copies(lay, dst, True):
            cp.wait()

    def all_rows(i):
        return i

    def k_blocks(k):
        return lambda i: i * 4 + k

    kx(0).start()
    kg(0).start()
    load(1, "down").start()
    load(1, "up").start()
    load(1, "down").wait()
    load(1, "up").wait()

    def hook1(p):
        if p == 2:
            kx(1).start()
            kg(1).start()

    own(1, gtop, hook1)
    kx(0).wait_recv()
    kg(0).wait_recv()
    fkx(0).start()
    fkg(0).start()
    add_quarter(1, gtop, g1, 0)
    ag[1]["x"](0).start()
    weights("down", down1, False, aa.at[1], gtop, 8, all_rows, False)
    add_quarter(1, gtop, g1, 1)
    ag[1]["x"](1).start()
    weights("up", up1, False, x1, dh.at[1], 8, all_rows, False)
    for s in range(2):
        sx0["y"](s).start()
    fkx(0).wait_recv()
    fkg(0).wait_recv()
    ag[1]["x"](0).wait_recv()
    ag[1]["f"](0).start()
    peer(1, xp1, gp2, 2, k_blocks(0))
    kx(1).wait_recv()
    kg(1).wait_recv()
    fkx(1).start()
    fkg(1).start()
    fkx(1).wait_recv()
    fkg(1).wait_recv()
    peer(1, xp1, gp2, 2, k_blocks(1))
    load(0, "down").start()
    load(0, "up").start()
    ag[1]["x"](1).wait_recv()
    ag[1]["f"](1).start()
    for s in range(2):
        ag[1]["c"](s).wait_recv()
    def pass_on(sh, s):
        sh["y"](s).wait_recv()
        sh["x"](s).start()
        sh["c"](s).start()

    def pass_core(sh, s):
        sh["x"](s).wait_recv()
        sh["f"](s).start()

    def have(s):
        for sh in (sx0, sg1):
            for kind in "cf":
                sh[kind](s).wait_recv()

    def hook0(p):
        if p == 1:
            pass_on(sx0, 1)
        if p == 2:
            pass_core(sx0, 0)

    pass_on(sx0, 0)
    for s in range(2):
        sg1["y"](s).start()
    load(0, "down").wait()
    load(0, "up").wait()
    own(0, g1, hook0)
    pass_on(sg1, 0)
    kx(2).start()
    kg(2).start()
    weights("down", down0, False, aa.at[0], g1, 8, all_rows, False)
    add_quarter(0, g1, g0, 0)
    weights("up", up0, False, x0, dh.at[0], 8, all_rows, False)
    pass_on(sg1, 1)
    r2_copy(0, 1).start()
    ag[0]["x"](0).start()
    pass_core(sx0, 1)
    early = lambda i: lax.div(i, 2) * 4 + lax.rem(i, 2)
    late = lambda i: lax.div(i, 2) * 4 + 2 + lax.rem(i, 2)
    weights("down", down1, True, ap.at[1], gp2, 4, early, False)
    pass_core(sg1, 0)
    kx(3).start()
    kg(3).start()
    have(0)
    peer(0, xp0, gp1, 4, lambda i: i * 2)
    pass_core(sg1, 1)
    kx(2).wait_recv()
    kg(2).wait_recv()
    fkx(2).start()
    fkg(2).start()
    have(1)
    peer(0, xp0, gp1, 4, lambda i: i * 2 + 1)
    load(1, "down").start()
    load(1, "up").start()
    add_quarter(0, g1, g0, 1)
    ag[0]["x"](1).start()
    fkx(2).wait_recv()
    fkg(2).wait_recv()
    load(1, "down").wait()
    load(1, "up").wait()
    peer(1, xp1, gp2, 2, k_blocks(2))
    weights("up", up1, True, xp1, dhp.at[1], 4, early, False)
    kx(3).wait_recv()
    kg(3).wait_recv()
    fkx(3).start()
    fkg(3).start()
    ag[0]["x"](0).wait_recv()
    ag[0]["f"](0).start()
    fkx(3).wait_recv()
    fkg(3).wait_recv()
    peer(1, xp1, gp2, 2, k_blocks(3))
    weights("down", down1, True, ap.at[1], gp2, 4, late, False)
    weights("up", up1, True, xp1, dhp.at[1], 4, late, False)
    ag[0]["x"](1).wait_recv()
    ag[0]["f"](1).start()
    for s in range(2):
        ag[0]["c"](s).wait_recv()
        ag[0]["f"](s).wait_recv()

    for k in range(4):
        for d in (kx, kg, fkx, fkg):
            d(k).wait_send()
    for l in range(2):
        for pair in range(4):
            r1_copy(l, pair).wait_send()
        for s in range(2):
            r2_copy(l, s).wait_send()
            for kind in "xcf":
                ag[l][kind](s).wait_send()
    for sh in (sx0, sg1):
        for kind in "yxcf":
            for s in range(2):
                sh[kind](s).wait_send()


N_COPIES = 64


def finish_kernel(xp0, gp1, dhp, ap, down0, up0, down1, up1, g0_in, g0, dw_up, dw_down, acc_d, acc_u, sem):
    dp = lax.axis_index("dp")
    tokens, width = g0_in.shape
    NB = width // 2
    blocks = tokens // BM
    ins = [pltpu.make_async_copy(src, dst, sem.at[i]) for i, (src, dst) in enumerate(((down0, acc_d), (up0, acc_u)))]
    for cp in ins:
        cp.start()

    def phase(kind, acc, lhs, rhs, moved, out, g_at):
        lw, rw = (NB, width) if kind == "up" else (width, NB)
        lcol, rcol = (dp, 0) if kind == "up" else (0, dp)
        rows = 2 * NB // blocks
        gb = tokens // (2 * blocks)

        def body(lr, rr, mr, gr, mo, go):
            dw_step(kind, acc, lr, rr)
            mo[...] = mr[0] if len(mr.shape) == 3 else mr[...]
            go[...] = gr[...]

        half = blocks // 2
        if kind == "up":
            out_spec = pl.BlockSpec((rows, NB), lambda i: (lax.rem(i, half), lax.div(i, half)))
        else:
            out_spec = pl.BlockSpec((rows, NB), lambda i: (i, 0))
        g_spec = pl.BlockSpec((gb, width), lambda i: (g_at * blocks + i, 0))
        pltpu.emit_pipeline(
            body, grid=(blocks,),
            in_specs=[
                pl.BlockSpec((BM, lw), lambda i: (i, lcol)),
                pl.BlockSpec((BM, rw), lambda i: (i, rcol)),
                pl.BlockSpec((1, rows, NB), lambda i: (lax.div(i, half), lax.rem(i, half), 0)),
                g_spec,
            ],
            out_specs=[out_spec, g_spec],
        )(lhs, rhs, moved, g0_in, out, g0.at[0])

    def put(kind, acc, dst):
        return [pltpu.make_async_copy(acc.at[i], halves(kind, dst, i, NB), sem.at[2 * (kind == "up") + i]) for i in range(2)]

    ins[0].wait()
    phase("down", acc_d, ap.at[0], gp1, down1, dw_down.at[1], 0)
    ins[1].wait()
    outs = put("down", acc_d, dw_down.at[0])
    for cp in outs:
        cp.start()
    phase("up", acc_u, xp0, dhp.at[0], up1, dw_up.at[1], 1)
    outs += put("up", acc_u, dw_up.at[0])
    for cp in outs[2:]:
        cp.start()
    for cp in outs:
        cp.wait()


def solution(mesh):
    def local_backward(w_up, w_down, saved_x, saved_h, grad_out):
        tokens, width = grad_out.shape[1:]
        row = jax.ShapeDtypeStruct((tokens, width), BF16)
        two = jax.ShapeDtypeStruct((2, tokens, width), BF16)
        half = jax.ShapeDtypeStruct((2, tokens // 2, width), BF16)
        quarter = jax.ShapeDtypeStruct((2, tokens // 4, width), BF16)
        sums = jax.ShapeDtypeStruct((2, width // 2, width // 2), F32)
        outs = [row, row, two, two, two, half, quarter, row, row, row, row, two, two, sums, sums, sums, sums]
        flops = 2 * tokens * width * width
        g0, g1, dh, aa, ps, r1, r2, xp1, gp2, xp0, gp1, dhp, ap, down1, up1, down0, up0 = pl.pallas_call(
            main_kernel,
            out_shape=outs,
            in_specs=[ANY] * 5,
            out_specs=[ANY] * len(outs),
            scratch_shapes=[
                pltpu.VMEM((width, width), BF16),
                pltpu.VMEM((width, width), BF16),
                pltpu.VMEM(sums.shape, F32),
                pltpu.SemaphoreType.DMA((2,)),
                pltpu.SemaphoreType.DMA((2,)),
                pltpu.SemaphoreType.DMA((N_COPIES,)),
                pltpu.SemaphoreType.DMA((N_COPIES,)),
            ],
            compiler_params=pltpu.CompilerParams(
                collective_id=0, has_side_effects=True, vmem_limit_bytes=VMEM_LIMIT),
            cost_estimate=pl.CostEstimate(flops=11 * flops, bytes_accessed=10**9, transcendentals=0),
            name="backward_main",
        )(w_up, w_down, saved_x, saved_h, grad_out)
        return tuple(pl.pallas_call(
            finish_kernel,
            out_shape=[
                jax.ShapeDtypeStruct((1, tokens, width), BF16),
                jax.ShapeDtypeStruct((2, width // 2, width), F32),
                jax.ShapeDtypeStruct((2, width, width // 2), F32),
            ],
            in_specs=[ANY] * 9,
            out_specs=[ANY] * 3,
            scratch_shapes=[
                pltpu.VMEM(sums.shape, F32),
                pltpu.VMEM(sums.shape, F32),
                pltpu.SemaphoreType.DMA((4,)),
            ],
            compiler_params=pltpu.CompilerParams(vmem_limit_bytes=VMEM_LIMIT),
            cost_estimate=pl.CostEstimate(flops=flops, bytes_accessed=3 * 10**8, transcendentals=0),
            name="backward_finish",
        )(xp0, gp1, dhp, ap, down0, up0, down1, up1, g0))

    return jax.shard_map(
        local_backward,
        mesh=mesh,
        in_specs=(P(None, None, "tp"), P(None, "tp", None), P(None, "dp", None, None), P(None, "dp", None, "tp"), P("dp", None, None)),
        out_specs=(P("dp", None, None), P(None, "dp", "tp"), P(None, "tp", "dp")),
        check_vma=False,
    )
```

```python
import math

import jax
import jax.numpy as jnp
from jax import lax
from jax.experimental import pallas as pl
from jax.experimental.pallas import tpu as pltpu
from jax.sharding import PartitionSpec as P

C0 = math.sqrt(2.0 / math.pi)
C1 = 0.044715
F32, BF16 = jnp.float32, jnp.bfloat16
ANY = pl.BlockSpec(memory_space=pl.ANY)
VMEM_LIMIT = 67043328
BM = 512


def gelu_and_slope(h):
    sq = h * h
    q = 0.5 + 0.5 * jnp.tanh(h * (C0 + (C0 * C1) * sq))
    act = h * q
    return act, q + act * (1.0 - q) * (2.0 * C0 + (6.0 * C0 * C1) * sq)


def dot(a, b, ca, cb):
    return lax.dot_general(a, b, (((ca,), (cb,)), ((), ())), preferred_element_type=F32)


def dw_step(kind, acc, lr, rr):
    n = acc.shape[1]
    for i in range(2):
        at = slice(i * n, i * n + n)
        if kind == "up":
            acc[i] += dot(lr[...], rr[:, at], 0, 0)
        else:
            acc[i] += dot(lr[:, at], rr[...], 0, 0)


def halves(kind, ref, i, n):
    at = pl.ds(i * n, n)
    return ref.at[:, at] if kind == "up" else ref.at[at]


def main_kernel(
    w_up, w_down, xs, hs, g2,
    g0, g1, dh, aa, ps, r2, xp1, gp2, xp0, gp1, dhp, ap, down1, up1, down0, up0,
    wu, wd, add_buf, wsem, asem, psem, send, recv,
):
    tokens, width = g2.shape[1:]
    dp, tp = lax.axis_index("dp"), lax.axis_index("tp")
    c, x = lax.rem(tp, 2), lax.div(tp, 2)
    Y, X, C = (1 - dp, tp), (dp, (1 - x) * 2 + c), (dp, x * 2 + (1 - c))
    half = tokens // 2
    quarter = tokens // 4
    sub = quarter // 2
    NB = width // 2

    def load(l, which):
        src, dst, i = (w_up, wu, 0) if which == "up" else (w_down, wd, 1)
        return pltpu.make_async_copy(src.at[l], dst, wsem.at[i])

    load(1, "down").start()
    load(1, "up").start()
    add_buf[1] = jnp.zeros(add_buf.shape[1:], BF16)
    barrier = pltpu.get_barrier_semaphore()
    for peer in (Y, X, C):
        pl.semaphore_signal(barrier, inc=1, device_id=peer, device_id_type=pl.DeviceIdType.MESH)
    pl.semaphore_wait(barrier, 3)

    slot = {}

    def rc(name, src, dst, to, s=0, n=1):
        if name not in slot:
            slot[name] = sum(v[1] for v in slot.values()), n
        i = slot[name][0] + s
        return pltpu.make_async_remote_copy(
            src_ref=src, dst_ref=dst, send_sem=send.at[i], recv_sem=recv.at[i],
            device_id=to, device_id_type=pl.DeviceIdType.MESH)

    def at_rows(ref, start, size):
        return ref.at[pl.ds(pl.multiple_of(start, sub), size)]

    def qrow(cc, xx, s):
        return cc * half + xx * quarter + s * sub

    def same(name, src, dst, row, to, s=0, n=1):
        return rc(name, at_rows(src, row, sub), at_rows(dst, row, sub), to, s, n)

    def k_row(k):
        return c * half + k * sub

    x1, x0, gtop = xs.at[1, 0], xs.at[0, 0], g2.at[0]

    def kx(k):
        return same(f"kx{k}", x1, xp1, k_row(k), Y)

    def kg(k):
        return same(f"kg{k}", gtop, gp2, k_row(k), Y)

    def fkx(k):
        return same(f"fkx{k}", xp1, xp1, k_row(k), C)

    def fkg(k):
        return same(f"fkg{k}", gp2, gp2, k_row(k), C)

    def share(tag, src, dst):
        return {
            "y": lambda s: same(f"{tag}y{s}", src, dst, qrow(c, x, s), Y),
            "x": lambda s: same(f"{tag}x{s}", dst, dst, qrow(c, x, s), X),
            "c": lambda s: same(f"{tag}c{s}", dst, dst, qrow(c, x, s), C),
            "f": lambda s: same(f"{tag}f{s}", dst, dst, qrow(c, 1 - x, s), C),
        }

    sx0 = share("sx0", x0, xp0)
    sg1 = share("sg1", g1, gp1)

    def gather(tag, g):
        return {
            "x": lambda s: same(f"{tag}x{s}", g, g, qrow(c, x, s), X),
            "c": lambda s: same(f"{tag}c{s}", g, g, qrow(c, x, s), C),
            "f": lambda s: same(f"{tag}f{s}", g, g, qrow(c, 1 - x, s), C),
        }

    ag = {1: gather("ag1", g1), 0: gather("ag0", g0)}

    def half_cols(m):
        return pl.ds(m * NB, NB)

    def r1_copy(l, pair, m, share_buf):
        return rc(f"r1_{l}", share_buf.at[m], add_buf.at[lax.rem(pair, 2), m], C, pair * 2 + m, 8)

    def r2_copy(l, s):
        return rc(f"r2_{l}", at_rows(ps.at[l], qrow(c, 1 - x, s), sub),
                  at_rows(r2.at[l], s * sub, sub), X, s, 2)

    def at_step(cond, hook):
        @pl.when(cond)
        def _():
            hook()

    def own(l, g, hooks, dh_even, dh_odd, share_buf):
        def place(i):
            pair, j = lax.div(i, 2), lax.rem(i, 2)
            xx = jnp.where(pair < 2, 1 - x, x)
            return pair, j, jnp.where(j == 0, 1 - c, c) * 4 + xx * 2 + lax.rem(pair, 2)

        def kept(blk, m):
            rows = pl.ds(pl.multiple_of(blk * BM, BM), BM)
            return pltpu.make_async_copy(share_buf.at[m], ps.at[l, rows, half_cols(m)], psem.at[m])

        def act_part(n, keep, gr, hr, dr, ar):
            at = pl.ds(pl.multiple_of(n * NB, NB), NB)
            d = dot(gr[...], wd[at, :], 1, 1)
            act, slope = gelu_and_slope(hr[...].astype(F32))
            d = (d * slope).astype(BF16)
            keep[:, at] = d
            dr[...] = d
            ar[...] = act.astype(BF16)

        def x_part(b, n, kept_dh):
            pair, j, _ = place(b)
            at = pl.ds(pl.multiple_of(n * NB, NB), NB)
            out = dot(kept_dh[...], wu[at, :], 1, 1)
            got = add_buf[jnp.where(j == 1, lax.rem(pair, 2), 1 - lax.rem(pair, 2)), n].astype(F32)
            share_buf[n] = (out + jnp.where(j == 1, got, 0.0)).astype(BF16)

        def body(gr, hr, dr, ar):
            i, n = pl.program_id(0), pl.program_id(1)
            b = i - 1
            pair, j, blk = place(b)

            @pl.when(jnp.logical_and(i > 0, j == 1))
            def _():
                r1_copy(l, pair, n, share_buf).wait_recv()
                r1_copy(l, pair, n, share_buf).wait_send()

            @pl.when(jnp.logical_and(j == 0, i > 1))
            def _():
                kept(place(b - 1)[2], n).wait()

                if l == 1:
                    @pl.when(jnp.logical_and(n == 1, pair - 1 < 2))
                    def _():
                        r2_copy(l, lax.rem(pair - 1, 2)).start()

            if l == 0:
                @pl.when(jnp.logical_and(i == 1, n == 0))
                def _():
                    ag[1]["f"](1).wait_recv()

            @pl.when(jnp.logical_and(i == 1, n == 0))
            def _():
                load(l, "up").wait()

            @pl.when(i == 0)
            def _():
                act_part(n, dh_even, gr, hr, dr, ar)

            for odd, (new, old) in enumerate(((dh_even, dh_odd), (dh_odd, dh_even))):
                @pl.when(jnp.logical_and(lax.rem(i, 2) == odd, jnp.logical_and(i > 0, i < 8)))
                def _():
                    act_part(n, new, gr, hr, dr, ar)
                    x_part(b, n, old)

            @pl.when(i == 8)
            def _():
                x_part(b, n, dh_odd)

            @pl.when(jnp.logical_and(i > 0, j == 0))
            def _():
                r1_copy(l, pair, n, share_buf).start()

            @pl.when(jnp.logical_and(i > 0, j == 1))
            def _():
                kept(blk, n).start()

            for at_i, hook in hooks.items():
                at_step(jnp.logical_and(i == at_i, n == 1), hook)

        def act_block(i):
            return place(jnp.minimum(i, 7))[2]

        tile = pl.BlockSpec((BM, NB), lambda i, n: (act_block(i), jnp.where(i == 8, 1, n)))
        pltpu.emit_pipeline(
            body, grid=(9, 2),
            in_specs=[pl.BlockSpec((BM, width), lambda i, n: (act_block(i), 0)), tile],
            out_specs=[tile, tile],
        )(g, hs.at[l, 0], dh.at[l], aa.at[l])
        for m in range(2):
            kept(place(7)[2], m).wait()

    def run_own(l, g, hooks):
        pl.run_scoped(
            lambda *bufs: own(l, g, hooks, *bufs),
            pltpu.VMEM((BM, width), BF16), pltpu.VMEM((BM, width), BF16), pltpu.VMEM((2, BM, NB), BF16))

    QB = 128

    def add_quarter(l, g, out, s):
        r2_copy(l, s).wait_recv()
        base = lax.div(qrow(c, x, s), QB)

        def body(gr, pr, rr, orf):
            orf[...] = (gr[...].astype(F32) + (pr[...].astype(F32) + rr[...].astype(F32))).astype(BF16)

        at = pl.BlockSpec((QB, width), lambda i: (base + i, 0))
        pltpu.emit_pipeline(
            body, grid=(sub // QB,),
            in_specs=[at, at, pl.BlockSpec((QB, width), lambda i: (s * (sub // QB) + i, 0))],
            out_specs=[at],
        )(g, ps.at[l], r2.at[l], out)
        ag[l]["c"](s).start()

    def peer(l, px, pg, blocks, row_block, hooks={}):
        def body(xr, gr, dr, ar):
            i, n = pl.program_id(0), pl.program_id(1)
            for at_i, hook in hooks.items():
                at_step(jnp.logical_and(i == at_i, n == 0), hook)
            t = pl.ds(pl.multiple_of(n * NB, NB), NB)
            pre = dot(xr[...], wu[:, t], 1, 0).astype(BF16)
            act, slope = gelu_and_slope(pre.astype(F32))
            ar[...] = act.astype(BF16)
            dr[...] = (dot(gr[...], wd[t, :], 1, 1) * slope).astype(BF16)

        full = pl.BlockSpec((BM, width), lambda i, n: (row_block(i), 0))
        tile = pl.BlockSpec((BM, NB), lambda i, n: (row_block(i), n))
        pltpu.emit_pipeline(body, grid=(blocks, 2), in_specs=[full, full], out_specs=[tile, tile])(
            px, pg, dhp.at[l], ap.at[l])

    pending = {0: [], 1: []}

    def acc_copies(acc, which, ref, out):
        pairs = [(acc.at[i], ref.at[i]) if out else (ref.at[i], acc.at[i]) for i in range(2)]
        return [pltpu.make_async_copy(*pair, asem.at[which * 2 + i]) for i, pair in enumerate(pairs)]

    def settle(which):
        for args in pending[which]:
            for cp in acc_copies(*args):
                cp.wait()
        pending[which] = []

    def move(acc, which, ref, out):
        settle(which)
        pending[which] = [(acc, which, ref, out)]
        for cp in acc_copies(acc, which, ref, out):
            cp.start()

    def weights(kind, acc, which, lhs, rhs, blocks, row_block, zero=False, hooks={}, split=False):
        settle(which)
        if zero:
            acc[...] = jnp.zeros_like(acc)
        up = kind == "up"
        if split:
            def body(lr, rr):
                i, n = pl.program_id(0), pl.program_id(1)
                for at_i, hook in hooks.items():
                    at_step(jnp.logical_and(i == at_i, n == 0), hook)
                acc[n] += dot(lr[...], rr[...], 0, 0)

            pltpu.emit_pipeline(
                body,
                grid=(blocks, 2),
                in_specs=[
                    pl.BlockSpec((BM, NB), lambda i, n: (row_block(i), dp if up else n)),
                    pl.BlockSpec((BM, NB), lambda i, n: (row_block(i), n if up else dp)),
                ],
            )(lhs, rhs)
            return
        lw, rw = (NB, width) if up else (width, NB)
        lcol, rcol = (dp, 0) if up else (0, dp)

        def body(lr, rr):
            i = pl.program_id(0)
            for at_i, hook in hooks.items():
                at_step(i == at_i, hook)
            dw_step(kind, acc, lr, rr)

        pltpu.emit_pipeline(
            body,
            grid=(blocks,),
            in_specs=[
                pl.BlockSpec((BM, lw), lambda i: (row_block(i), lcol)),
                pl.BlockSpec((BM, rw), lambda i: (row_block(i), rcol)),
            ],
        )(lhs, rhs)

    def all_rows(i):
        return i

    def k_blocks(k):
        return lambda i: i * 4 + k

    def go(*copies):
        for cp in copies:
            cp.start()

    def pass_on(sh, s):
        sh["y"](s).wait_recv()
        go(sh["x"](s), sh["c"](s))

    def pass_core(sh, s):
        sh["x"](s).wait_recv()
        go(sh["f"](s))

    def pass_k(k):
        for d in (kx, kg):
            d(k).wait_recv()
        go(fkx(k), fkg(k))

    def have_k(k):
        for d in (fkx, fkg):
            d(k).wait_recv()

    def have(s):
        for sh in (sx0, sg1):
            for kind in "cf":
                sh[kind](s).wait_recv()

    def early(i):
        return lax.div(i, 2) * 4 + lax.rem(i, 2)

    def late(i):
        return lax.div(i, 2) * 4 + 2 + lax.rem(i, 2)

    go(kx(0), kg(0))
    load(1, "down").wait()
    run_own(1, gtop, {4: lambda: go(kx(1), kg(1))})
    pass_k(0)
    add_quarter(1, gtop, g1, 0)
    go(ag[1]["x"](0))

    def block1_own(acc):
        weights("down", acc, 0, aa.at[1], gtop, 8, all_rows, True)
        move(acc, 0, down1, True)
        add_quarter(1, gtop, g1, 1)
        go(ag[1]["x"](1), sx0["y"](0), sg1["y"](0))
        weights("up", acc, 0, x1, dh.at[1], 8, all_rows, True)
        move(acc, 0, up1, True)
        go(sx0["y"](1), sg1["y"](1))
        settle(0)

    pl.run_scoped(block1_own, pltpu.VMEM((2, NB, NB), F32))
    have_k(0)

    def on_k1():
        ag[1]["x"](0).wait_recv()
        go(ag[1]["f"](0))
        pass_k(1)

    peer(1, xp1, gp2, 2, k_blocks(0), {1: on_k1})
    have_k(1)
    peer(1, xp1, gp2, 2, k_blocks(1))
    go(load(0, "down"), load(0, "up"))
    ag[1]["x"](1).wait_recv()
    go(ag[1]["f"](1))
    for s in range(2):
        ag[1]["c"](s).wait_recv()
    ag[1]["f"](0).wait_recv()
    pass_on(sx0, 0)
    load(0, "down").wait()

    def own0_late():
        pass_core(sx0, 0)
        go(r2_copy(0, 0))

    run_own(0, g1, {4: lambda: pass_on(sg1, 0), 6: own0_late})
    go(kx(2), kg(2))

    def with_acc(fn):
        pl.run_scoped(fn, pltpu.VMEM((2, NB, NB), F32))

    def down_own(acc):
        weights("down", acc, 0, aa.at[0], g1, 8, all_rows, True,
                {1: lambda: pass_on(sx0, 1), 5: lambda: pass_core(sg1, 0)})
        move(acc, 0, down0, True)
        settle(0)

    def on_s1():
        pass_on(sg1, 1)
        go(r2_copy(0, 1), kx(3), kg(3))

    def up_own(acc):
        weights("up", acc, 0, x0, dh.at[0], 8, all_rows, True, {6: lambda: pass_core(sx0, 1)})
        move(acc, 0, up0, True)
        move(acc, 0, down1, False)
        weights("down", acc, 0, ap.at[1], gp2, 4, early)
        move(acc, 0, down1, True)
        settle(0)

    def down_late(acc):
        move(acc, 0, down1, False)
        weights("down", acc, 0, ap.at[1], gp2, 4, late)
        move(acc, 0, down1, True)
        ag[0]["x"](1).wait_recv()
        go(ag[0]["f"](1))
        settle(0)

    with_acc(down_own)
    have(0)
    peer(0, xp0, gp1, 4, lambda i: i * 2, {2: on_s1})
    add_quarter(0, g1, g0, 0)
    go(ag[0]["x"](0))
    with_acc(up_own)
    pass_core(sg1, 1)
    have(1)
    peer(0, xp0, gp1, 4, lambda i: i * 2 + 1, {2: lambda: pass_k(2)})
    go(load(1, "up"), load(1, "down"))
    add_quarter(0, g1, g0, 1)
    go(ag[0]["x"](1))
    have_k(2)
    load(1, "up").wait()
    load(1, "down").wait()
    peer(1, xp1, gp2, 2, k_blocks(2), {1: lambda: pass_k(3)})
    have_k(3)
    peer(1, xp1, gp2, 2, k_blocks(3))
    ag[0]["x"](0).wait_recv()
    go(ag[0]["f"](0))
    with_acc(down_late)
    for s in range(2):
        ag[0]["c"](s).wait_recv()
        ag[0]["f"](s).wait_recv()

    for k in range(4):
        for d in (kx, kg, fkx, fkg):
            d(k).wait_send()
    for l in range(2):
        for s in range(2):
            r2_copy(l, s).wait_send()
            for kind in "xcf":
                ag[l][kind](s).wait_send()
    for sh in (sx0, sg1):
        for kind in "yxcf":
            for s in range(2):
                sh[kind](s).wait_send()


N_COPIES = 72


def finish_kernel(
    xp0, gp1, xp1, gp2, dhp, ap, down0, up0, down1, up1, g0_in,
    g0, dw_up, dw_down,
    acc_d, acc_u, acc_l, mbuf, gbuf, sem, msem, ssem, bsem,
):
    dp = lax.axis_index("dp")
    tokens, width = g0_in.shape
    NB = width // 2
    blocks = tokens // BM

    def acc_in(acc, src, which):
        return [pltpu.make_async_copy(src.at[i], acc.at[i], sem.at[which * 2 + i]) for i in range(2)]

    def acc_out(kind, acc, dst, which):
        return [pltpu.make_async_copy(acc.at[i], halves(kind, dst, i, NB), sem.at[which * 2 + i]) for i in range(2)]

    def start(copies):
        for cp in copies:
            cp.start()

    def wait(copies):
        for cp in copies:
            cp.wait()

    piece = NB // 8

    def strip_in(acc, src, p, sem):
        h, r = lax.div(p, 8), pl.multiple_of(lax.rem(p, 8) * piece, piece)
        return pltpu.make_async_copy(src.at[h, pl.ds(r, piece)], acc.at[h, pl.ds(r, piece)], sem)

    def strip_out(kind, acc, dst, p, sem):
        h, r = lax.div(p, 8), pl.multiple_of(lax.rem(p, 8) * piece, piece)
        if kind == "up":
            far = dst.at[pl.ds(r, piece), pl.ds(pl.multiple_of(h * NB, NB), NB)]
        else:
            far = dst.at[pl.ds(pl.multiple_of(p * piece, piece), piece)]
        return pltpu.make_async_copy(acc.at[h, pl.ds(r, piece)], far, sem)

    def phase(kind, acc, lhs, rhs, steps, row_block, g_first, moves_m, ins, outs):
        lw, rw = (NB, width) if kind == "up" else (width, NB)
        lcol, rcol = (dp, 0) if kind == "up" else (0, dp)
        per = 16 // steps
        gb = tokens // 16

        def g_move(i, out_side):
            slot = lax.rem(i, 2)
            rows = pl.ds(pl.multiple_of((g_first + i) * gb, gb), gb)
            if out_side:
                return pltpu.make_async_copy(gbuf.at[slot], g0.at[0, rows], msem.at[1, slot])
            return pltpu.make_async_copy(g0_in.at[rows], gbuf.at[slot], msem.at[0, slot])

        def m_move(p, out_side):
            slot = lax.rem(p, 4)
            h, r = lax.div(p, 8), pl.multiple_of(lax.rem(p, 8) * piece, piece)
            if out_side:
                far = dw_down.at[1, pl.ds(pl.multiple_of(p * piece, piece), piece)]
                return pltpu.make_async_copy(mbuf.at[slot], far, bsem.at[1, slot])
            return pltpu.make_async_copy(down1.at[h, pl.ds(r, piece)], mbuf.at[slot], bsem.at[0, slot])

        def m_pair(i):
            return [i * 2, i * 2 + 1] if moves_m else []

        def strips(i):
            res = []
            for k in range(per):
                for args in ins:
                    res.append(strip_in(*args, i * per + k, ssem.at[len(res)]))
                for args in outs:
                    res.append(strip_out(*args, i * per + k, ssem.at[len(res)]))
            return res

        moves_g = g_first is not None
        if moves_g:
            g_move(0, False).start()
        start([m_move(p, False) for p in m_pair(0)])

        def body(lr, rr):
            i = pl.program_id(0)

            @pl.when(i > 0)
            def _():
                wait(strips(i - 1))

            start(strips(i))
            wait([m_move(p, False) for p in m_pair(i)])
            start([m_move(p, True) for p in m_pair(i)])
            if moves_m:
                @pl.when(i > 0)
                def _():
                    wait([m_move(p, True) for p in m_pair(i - 1)])

                @pl.when(i < steps - 1)
                def _():
                    start([m_move(p, False) for p in m_pair(i + 1)])
            if moves_g:
                g_move(i, False).wait()
                g_move(i, True).start()

                @pl.when(i > 0)
                def _():
                    g_move(i - 1, True).wait()

                @pl.when(i < steps - 1)
                def _():
                    g_move(i + 1, False).start()

            dw_step(kind, acc, lr, rr)

        pltpu.emit_pipeline(
            body, grid=(steps,),
            in_specs=[
                pl.BlockSpec((BM, lw), lambda i: (row_block(i), lcol)),
                pl.BlockSpec((BM, rw), lambda i: (row_block(i), rcol)),
            ],
        )(lhs, rhs)
        wait(strips(steps - 1))
        wait([m_move(p, True) for p in m_pair(steps - 1)])
        if moves_g:
            g_move(steps - 1, True).wait()

    every = lambda i: i
    start(acc_in(acc_d, down0, 0))
    wait(acc_in(acc_d, down0, 0))
    phase("down", acc_d, ap.at[0], gp1, blocks, every, 0, True, [(acc_u, up0)], [])
    phase("up", acc_u, xp0, dhp.at[0], blocks, every, blocks, False, [(acc_l, up1)], [("down", acc_d, dw_down.at[0])])
    phase("up", acc_l, xp1, dhp.at[1], blocks, every, None, False, [], [("up", acc_u, dw_up.at[0])])
    start(acc_out("up", acc_l, dw_up.at[1], 1))
    wait(acc_out("up", acc_l, dw_up.at[1], 1))


def solution(mesh):
    def local_backward(w_up, w_down, saved_x, saved_h, grad_out):
        tokens, width = grad_out.shape[1:]
        row = jax.ShapeDtypeStruct((tokens, width), BF16)
        two = jax.ShapeDtypeStruct((2, tokens, width), BF16)
        quarter = jax.ShapeDtypeStruct((2, tokens // 4, width), BF16)
        sums = jax.ShapeDtypeStruct((2, width // 2, width // 2), F32)
        outs = [row, row, two, two, two, quarter, row, row, row, row, two, two, sums, sums, sums, sums]
        flops = 2 * tokens * width * width
        g0, g1, dh, aa, ps, r2, xp1, gp2, xp0, gp1, dhp, ap, down1, up1, down0, up0 = pl.pallas_call(
            main_kernel,
            out_shape=outs,
            in_specs=[ANY] * 5,
            out_specs=[ANY] * len(outs),
            scratch_shapes=[
                pltpu.VMEM((width, width), BF16),
                pltpu.VMEM((width, width), BF16),
                pltpu.VMEM((2, 2, BM, width // 2), BF16),
                pltpu.SemaphoreType.DMA((2,)),
                pltpu.SemaphoreType.DMA((4,)),
                pltpu.SemaphoreType.DMA((2,)),
                pltpu.SemaphoreType.DMA((N_COPIES,)),
                pltpu.SemaphoreType.DMA((N_COPIES,)),
            ],
            compiler_params=pltpu.CompilerParams(
                collective_id=0, has_side_effects=True, vmem_limit_bytes=VMEM_LIMIT),
            cost_estimate=pl.CostEstimate(flops=11 * flops, bytes_accessed=10**9, transcendentals=0),
            name="backward_main",
        )(w_up, w_down, saved_x, saved_h, grad_out)
        return tuple(pl.pallas_call(
            finish_kernel,
            out_shape=[
                jax.ShapeDtypeStruct((1, tokens, width), BF16),
                jax.ShapeDtypeStruct((2, width // 2, width), F32),
                jax.ShapeDtypeStruct((2, width, width // 2), F32),
            ],
            in_specs=[ANY] * 11,
            out_specs=[ANY] * 3,
            scratch_shapes=[
                pltpu.VMEM(sums.shape, F32),
                pltpu.VMEM(sums.shape, F32),
                pltpu.VMEM(sums.shape, F32),
                pltpu.VMEM((4, width // 16, width // 2), F32),
                pltpu.VMEM((2, BM // 2, width), BF16),
                pltpu.SemaphoreType.DMA((4,)),
                pltpu.SemaphoreType.DMA((2, 2)),
                pltpu.SemaphoreType.DMA((8,)),
                pltpu.SemaphoreType.DMA((2, 4)),
            ],
            compiler_params=pltpu.CompilerParams(vmem_limit_bytes=VMEM_LIMIT),
            cost_estimate=pl.CostEstimate(flops=flops, bytes_accessed=3 * 10**8, transcendentals=0),
            name="backward_finish",
        )(xp0, gp1, xp1, gp2, dhp, ap, down0, up0, down1, up1, g0))

    return jax.shard_map(
        local_backward,
        mesh=mesh,
        in_specs=(P(None, None, "tp"), P(None, "tp", None), P(None, "dp", None, None), P(None, "dp", None, "tp"), P("dp", None, None)),
        out_specs=(P("dp", None, None), P(None, "dp", "tp"), P(None, "tp", "dp")),
        check_vma=False,
    )
```
